32 devices in a mesh: dp: 4 (over y, x), mp: 8 (over z, core).
Axes of the slice: x: 2, y: 2, z: 4, core: 2. Of those that a mesh axis runs over, the one named last changes fastest.
Arguments:
- tokens: bfloat16 [4, 1024, 5120], P('dp', 'mp'), may hold values from -6 to 6
- ln_gain: float32 [5120], replicated, may hold values from 0.1 to 1.9
- ln_bias: float32 [5120], replicated, may hold values from -3 to 3
- w_qkv: bfloat16 [5120, 3, 4096], P(None, None, 'mp'), may hold values from -0.15625 to 0.15625
- w_out: bfloat16 [4096, 5120], P('mp'), may hold values from -0.09375 to 0.09375
- grad_partial: bfloat16 [4, 4096, 5120], P('dp', 'mp'), may hold values from -6 to 6
Outputs:
- mixed: bfloat16 [4, 1024, 5120], P('dp', 'mp')
- grad_sum: float32 [4096, 5120], P('mp')
The draws below stay inside these ranges and needn't reach their ends.
All inputs are finite; a program needn't handle non-finite values.
Results may differ from the reference program's by a relative error of at most 0.014.
The reference program's roundings to bfloat16 on the way (of `normed`, `qkv`, `attn` and `context`) count: a program that leaves them out, or rounds other values in their place, can miss the bound.
Values may be sent and summed in bfloat16 or wider, within the bound.
A program may use at most 192 MiB of HBM per device.

```python
import jax
import jax.numpy as jnp
from jax import lax

D = 5120
HEAD = 128
HEADS = 32
SEQ = 128
IMG = 8
INNER = 4096
TOKENS = 1024
GROUPS = 4
N_MP = 8


def levels(key, shape, cuts, smallest, top_value):
    loudness = 1.0
    for dim, blocks in cuts:
        heights = jax.random.uniform(jax.random.fold_in(jax.random.fold_in(key, 6), dim), (blocks,), jnp.float32, smallest / len(cuts), top_value / len(cuts))
        loudness = loudness * jnp.repeat(jnp.exp(heights), shape[dim] // blocks).reshape((-1,) + (1,) * (len(shape) - 1 - dim))
    return loudness


def noise(rng, shape, scale, bound, shards=(), dtype=jnp.bfloat16):
    gain = levels(rng, shape, shards, -0.22, 0.18) if shards else 1.0
    drawn = jax.random.normal(rng, shape, jnp.float32) * scale * gain
    return jnp.minimum(jnp.maximum(drawn, -bound), bound).astype(dtype)


def setup_inputs(seed: int = 0) -> dict:
    streams_of = jax.random.split(jax.random.key(seed), 7)
    tokens = noise(streams_of[0], (GROUPS, TOKENS, D), 1.0, 6.0, ((0, 4), (1, 8)))
    ln_gain = jnp.clip(1.0 + 0.18 * jax.random.normal(streams_of[1], (D,), jnp.float32), 0.1, 1.9)
    ln_bias = noise(streams_of[2], (D,), 0.5, 3.0, (), jnp.float32)
    w_qkv = noise(streams_of[3], (D, 3, INNER), (D // 4) ** -0.5, 0.15625, ((2, 8),))
    w_out = noise(streams_of[4], (INNER, D), INNER ** -0.5, 0.09375, ((0, 8),))
    grad_partial = noise(streams_of[5], (GROUPS, INNER, D), 1.0, 6.0, ((0, 4), (1, 8)))
    return {"tokens": tokens, "ln_gain": ln_gain, "ln_bias": ln_bias, "w_qkv": w_qkv, "w_out": w_out, "grad_partial": grad_partial}


def layer_norm(rows, ln_gain, ln_bias):
    values = rows.astype(jnp.float32)
    center = lax.optimization_barrier(jnp.mean(values, axis=-1, keepdims=True))
    spread = lax.optimization_barrier(jnp.mean((values - center) * (values - center), axis=-1, keepdims=True))
    return ((values - center) * lax.rsqrt(spread + 1e-06) * ln_gain + ln_bias).astype(jnp.bfloat16)

def one_group(rows, ln_gain, ln_bias, w_qkv, w_out):
    normed = layer_norm(rows, ln_gain, ln_bias)
    qkv = jnp.dot(normed, w_qkv.reshape(D, 3 * INNER), preferred_element_type=jnp.float32).astype(jnp.bfloat16)
    query = qkv[:, :INNER].reshape(IMG, SEQ, HEADS, HEAD).astype(jnp.float32)
    keys = qkv[:, INNER:2 * INNER].reshape(IMG, SEQ, HEADS, HEAD).astype(jnp.float32)
    values = qkv[:, 2 * INNER:].reshape(IMG, SEQ, HEADS, HEAD).astype(jnp.float32)
    scores = jnp.einsum('bqhd,bkhd->bhqk', query, keys) * HEAD ** (-0.5)
    scaled = scores - lax.optimization_barrier(jnp.max(scores, axis=-1, keepdims=True))
    expsc = jnp.exp(scaled)
    attn = (expsc / lax.optimization_barrier(jnp.sum(expsc, axis=-1, keepdims=True))).astype(jnp.bfloat16)
    context = jnp.einsum('bhqk,bkhd->bqhd', attn.astype(jnp.float32), values).astype(jnp.bfloat16)
    context = context.reshape(TOKENS, INNER)
    width = INNER // N_MP

    def add_group(index, total):
        start = (index * width).astype(jnp.int32)
        cols = lax.dynamic_slice_in_dim(context, start, width, 1)
        wrows = lax.dynamic_slice_in_dim(w_out, start, width, 0)
        partial_sum = jnp.dot(cols, wrows, preferred_element_type=jnp.float32).astype(jnp.bfloat16)
        partial_sum = lax.optimization_barrier(partial_sum)
        return total + partial_sum.astype(jnp.float32)
    proj = lax.fori_loop(0, N_MP, add_group, jnp.zeros((TOKENS, D), jnp.float32))
    return (rows.astype(jnp.float32) + proj).astype(jnp.bfloat16)

def reference(tokens, ln_gain, ln_bias, w_qkv, w_out, grad_partial):
    mixed = lax.map(lambda rows: one_group(rows, ln_gain, ln_bias, w_qkv, w_out), tokens)
    grad_sum = lax.optimization_barrier(jnp.sum(grad_partial.astype(jnp.float32), axis=0))
    return (mixed, grad_sum)
```

```python
import functools

import jax
import jax.numpy as jnp
from jax import lax
from jax.experimental import pallas as pl
from jax.experimental.pallas import tpu as pltpu
from jax.sharding import PartitionSpec as P

HEAD = 128
SEQ = 128
TILE = 256
PIECES = 4
MESH = pl.DeviceIdType.MESH


def layer_norm(rows, ln_gain, ln_bias):
    values = rows.astype(jnp.float32)
    center = jnp.mean(values, axis=-1, keepdims=True)
    spread = jnp.mean((values - center) * (values - center), axis=-1, keepdims=True)
    return ((values - center) * lax.rsqrt(spread + 1e-06) * ln_gain + ln_bias).astype(jnp.bfloat16)


def kernel(
    n,
    normed,
    tokens,
    wq_hbm,
    wo_hbm,
    out,
    wq,
    wo,
    blocks,
    part,
    theirs,
    chain,
    qkv,
    ctx,
    load_sem,
    up_send,
    up_recv,
    dn_send,
    dn_recv,
    pr_send,
    pr_recv,
    pp_send,
    pp_recv,
    cu_send,
    cu_recv,
    cd_send,
    cd_recv,
):
    chips = n // 2
    me = lax.axis_index("mp")
    c = me // 2
    s = me % 2
    mate = c * 2 + 1 - s
    above = me + 2
    below = me - 2
    up = jnp.minimum(chips - 1 - c, 1)
    dn = jnp.minimum(c, 1)
    has_up = up > 0
    has_dn = dn > 0
    rows, width = normed.shape
    inner = wo_hbm.shape[0]
    wide = width // PIECES

    def remote(src, dst, send, recv, target):
        return pltpu.make_async_remote_copy(
            src_ref=src,
            dst_ref=dst,
            send_sem=send,
            recv_sem=recv,
            device_id={"mp": target},
            device_id_type=MESH,
        )

    load_q = pltpu.make_async_copy(wq_hbm, wq, load_sem.at[0])
    load_o = pltpu.make_async_copy(wo_hbm, wo, load_sem.at[1])
    load_x = pltpu.make_async_copy(normed, blocks.at[me], load_sem.at[2])
    load_q.start()
    load_o.start()
    load_x.start()

    barrier = pltpu.get_barrier_semaphore()
    pl.semaphore_signal(barrier, inc=1, device_id={"mp": mate}, device_id_type=MESH)

    @pl.when(has_up)
    def _():
        pl.semaphore_signal(barrier, inc=1, device_id={"mp": above}, device_id_type=MESH)

    @pl.when(has_dn)
    def _():
        pl.semaphore_signal(barrier, inc=1, device_id={"mp": below}, device_id_type=MESH)

    pl.semaphore_wait(barrier, 1 + up + dn)

    def block_up(src, slot, d):
        return remote(src, blocks.at[slot], up_send.at[d], up_recv.at[d], above)

    def block_dn(src, slot, d):
        return remote(src, blocks.at[slot], dn_send.at[d], dn_recv.at[d], below)

    def block_mate(src, slot, d, k):
        return remote(src, blocks.at[slot], pr_send.at[d, k], pr_recv.at[d, k], mate)

    def share_mate(slot, d, k):
        return remote(blocks.at[slot], theirs.at[k], pp_send.at[d, k], pp_recv.at[d, k], mate)

    def cols(q):
        return slice(q * wide, (q + 1) * wide)

    def sum_up(t, q):
        return remote(
            part.at[t, :, cols(q)], chain.at[t, :, cols(q)], cu_send.at[t, q], cu_recv.at[t, q], above
        )

    def sum_dn(t, q):
        slot = jnp.where(t == c - 1, chips, t)
        return remote(
            part.at[t, :, cols(q)], chain.at[slot, :, cols(q)], cd_send.at[t, q], cd_recv.at[t, q], below
        )

    @pl.when(has_up)
    def _():
        block_up(normed, me, 0).start()

    @pl.when(has_dn)
    def _():
        block_dn(normed, me, 0).start()

    block_mate(normed, me, 0, 0).start()
    load_x.wait()
    load_q.wait()
    load_o.wait()

    per_part = inner // TILE

    def attend(slot):
        def project(j, carry):
            which = j // per_part
            at = pl.multiple_of((j % per_part) * TILE, TILE)
            product = jnp.dot(
                blocks[slot], wq[which, :, pl.ds(at, TILE)], preferred_element_type=jnp.float32
            )
            qkv[which, :, pl.ds(at, TILE)] = product.astype(jnp.bfloat16)
            return carry

        lax.fori_loop(0, 3 * per_part, project, 0)
        for image in range(rows // SEQ):
            here = slice(image * SEQ, (image + 1) * SEQ)
            for h in range(inner // HEAD):
                lanes = slice(h * HEAD, (h + 1) * HEAD)
                scores = lax.dot_general(
                    qkv[0, here, lanes],
                    qkv[1, here, lanes],
                    (((1,), (1,)), ((), ())),
                    preferred_element_type=jnp.float32,
                ) * HEAD ** (-0.5)
                expsc = jnp.exp(scores - jnp.max(scores, axis=-1, keepdims=True))
                attn = (expsc / jnp.sum(expsc, axis=-1, keepdims=True)).astype(jnp.bfloat16)
                ctx[here, lanes] = jnp.dot(
                    attn, qkv[2, here, lanes], preferred_element_type=jnp.float32
                ).astype(jnp.bfloat16)

    def output(at):
        return jnp.dot(
            ctx[...], wo[:, pl.ds(at, TILE)], preferred_element_type=jnp.float32
        ).astype(jnp.bfloat16)

    def chain_step(e):
        @pl.when(dn * jnp.maximum(e - c, 0) > 0)
        def _():
            for q in range(PIECES):
                sum_up(e, q).wait_recv()
                part[e, :, cols(q)] = (
                    part[e, :, cols(q)].astype(jnp.float32) + chain[e, :, cols(q)].astype(jnp.float32)
                ).astype(jnp.bfloat16)
                sum_up(e, q).start()

        t = chips - 1 - e

        @pl.when(up * jnp.maximum(c - t, 0) > 0)
        def _():
            for q in range(PIECES):
                remote(
                    part.at[t, :, cols(q)],
                    chain.at[t, :, cols(q)],
                    cd_send.at[t, q],
                    cd_recv.at[t, q],
                    below,
                ).wait_recv()
                part[t, :, cols(q)] = (
                    part[t, :, cols(q)].astype(jnp.float32) + chain[t, :, cols(q)].astype(jnp.float32)
                ).astype(jnp.bfloat16)
                sum_dn(t, q).start()

    def step(d, carry):
        lo = c - d
        hi = c + d
        lo_ok = jnp.minimum(jnp.maximum(lo + 1, 0), 1)
        hi_ok = jnp.minimum(jnp.maximum(chips - hi, 0), jnp.minimum(d, 1))

        @pl.when(lo_ok * d > 0)
        def _():
            slot = lo * 2 + s
            block_up(blocks.at[slot], slot, d - 1).wait_recv()

            @pl.when(up + d * 0 > 0)
            def _():
                block_up(blocks.at[slot], slot, d).start()

            block_mate(blocks.at[slot], slot, d, 0).start()

        @pl.when(hi_ok > 0)
        def _():
            slot = hi * 2 + s
            block_dn(blocks.at[slot], slot, d - 1).wait_recv()

            @pl.when(dn + d * 0 > 0)
            def _():
                block_dn(blocks.at[slot], slot, d).start()

            block_mate(blocks.at[slot], slot, d, 1).start()

        def one(i, inner_carry):
            k = i % 2
            own = i // 2
            t = jnp.where(k == 0, lo, hi)

            @pl.when(jnp.where(k == 0, lo_ok, hi_ok) > 0)
            def _():
                slot = t * 2 + jnp.where(own == 1, s, 1 - s)

                @pl.when(own == 0)
                def _():
                    block_mate(blocks.at[slot], slot, d, k).wait_recv()

                attend(slot)

                @pl.when(own == 0)
                def _():
                    def put(j, inside):
                        at = pl.multiple_of(j * TILE, TILE)
                        blocks[slot, :, pl.ds(at, TILE)] = output(at)
                        return inside

                    lax.fori_loop(0, width // TILE, put, 0)
                    share_mate(slot, d, k).start()

                @pl.when(own == 1)
                def _():
                    share_mate(slot, d, k).wait_recv()

                    def put(j, inside):
                        at = pl.multiple_of(j * TILE, TILE)
                        both = output(at).astype(jnp.float32) + theirs[k, :, pl.ds(at, TILE)].astype(
                            jnp.float32
                        )
                        part[t, :, pl.ds(at, TILE)] = both.astype(jnp.bfloat16)
                        return inside

                    lax.fori_loop(0, width // TILE, put, 0)

                    @pl.when((1 - dn) * t > 0)
                    def _():
                        for q in range(PIECES):
                            sum_up(t, q).start()

                    @pl.when((1 - up) * (chips - 1 - t) > 0)
                    def _():
                        for q in range(PIECES):
                            sum_dn(t, q).start()

            return inner_carry

        lax.fori_loop(0, 4, one, 0)

        @pl.when(d >= 2)
        def _():
            chain_step(d - 1)

        return carry

    lax.fori_loop(0, chips, step, 0)
    if chips > 1:
        chain_step(chips - 1)

    @pl.when(has_up)
    def _():
        for q in range(PIECES):
            remote(
                part.at[c, :, cols(q)],
                chain.at[chips, :, cols(q)],
                cd_send.at[c, q],
                cd_recv.at[c, q],
                below,
            ).wait_recv()

    @pl.when(has_dn)
    def _():
        for q in range(PIECES):
            sum_up(c, q).wait_recv()

    def total(from_dn, from_up):
        for q in range(PIECES):
            value = part[c, :, cols(q)].astype(jnp.float32)
            if from_dn:
                value = value + chain[c, :, cols(q)].astype(jnp.float32)
            if from_up:
                value = value + chain[chips, :, cols(q)].astype(jnp.float32)
            out[:, cols(q)] = (tokens[:, cols(q)].astype(jnp.float32) + value).astype(jnp.bfloat16)

    @pl.when(dn * up > 0)
    def _():
        total(True, True)

    @pl.when(dn * (1 - up) > 0)
    def _():
        total(True, False)

    @pl.when((1 - dn) * up > 0)
    def _():
        total(False, True)

    @pl.when((1 - dn) * (1 - up) > 0)
    def _():
        total(False, False)

    def drain(d, carry):
        hi_ok = jnp.minimum(jnp.maximum(chips - c - d, 0), jnp.minimum(d, 1))

        @pl.when(c - d >= 0)
        def _():
            slot = (c - d) * 2 + s
            other = (c - d) * 2 + 1 - s

            @pl.when(up + d * 0 > 0)
            def _():
                block_up(blocks.at[slot], slot, d).wait_send()

            block_mate(blocks.at[slot], slot, d, 0).wait_send()
            share_mate(other, d, 0).wait_send()

        @pl.when(jnp.maximum(chips - c - d, 0) * dn > 0)
        def _():
            slot = (c + d) * 2 + s
            block_dn(blocks.at[slot], slot, d).wait_send()

        @pl.when(hi_ok > 0)
        def _():
            slot = (c + d) * 2 + s
            other = (c + d) * 2 + 1 - s
            block_mate(blocks.at[slot], slot, d, 1).wait_send()
            share_mate(other, d, 1).wait_send()

        @pl.when(d > c)
        def _():
            for q in range(PIECES):
                sum_up(d, q).wait_send()

        @pl.when(d < c)
        def _():
            for q in range(PIECES):
                sum_dn(d, q).wait_send()

        return carry

    lax.fori_loop(0, chips, drain, 0)


def body(n, tokens, ln_gain, ln_bias, w_qkv, w_out, grad_partial):
    local_rows = tokens[0]
    rows, width = local_rows.shape
    inner = w_out.shape[0]
    chips = n // 2
    normed = layer_norm(local_rows, ln_gain, ln_bias)
    dma = pltpu.SemaphoreType.DMA
    flops = 2 * rows * n * width * inner * 4
    mixed = pl.pallas_call(
        functools.partial(kernel, n),
        out_shape=jax.ShapeDtypeStruct((rows, width), jnp.bfloat16),
        in_specs=[
            pl.BlockSpec(memory_space=pl.ANY),
            pl.BlockSpec(memory_space=pltpu.VMEM),
            pl.BlockSpec(memory_space=pl.ANY),
            pl.BlockSpec(memory_space=pl.ANY),
        ],
        out_specs=pl.BlockSpec(memory_space=pltpu.VMEM),
        scratch_shapes=[
            pltpu.VMEM((3, width, inner), jnp.bfloat16),
            pltpu.VMEM((inner, width), jnp.bfloat16),
            pltpu.VMEM((n, rows, width), jnp.bfloat16),
            pltpu.VMEM((chips, rows, width), jnp.bfloat16),
            pltpu.VMEM((2, rows, width), jnp.bfloat16),
            pltpu.VMEM((chips + 1, rows, width), jnp.bfloat16),
            pltpu.VMEM((3, rows, inner), jnp.bfloat16),
            pltpu.VMEM((rows, inner), jnp.bfloat16),
            dma((3,)),
            dma((chips,)),
            dma((chips,)),
            dma((chips,)),
            dma((chips,)),
            dma((chips, 2)),
            dma((chips, 2)),
            dma((chips, 2)),
            dma((chips, 2)),
            dma((chips, PIECES)),
            dma((chips, PIECES)),
            dma((chips, PIECES)),
            dma((chips, PIECES)),
        ],
        compiler_params=pltpu.CompilerParams(
            collective_id=0, has_side_effects=True, vmem_limit_bytes=66_000_000
        ),
        cost_estimate=pl.CostEstimate(
            flops=flops * 8, bytes_accessed=300_000_000, transcendentals=0
        ),
    )(normed, local_rows, jnp.transpose(w_qkv, (1, 0, 2)), w_out)[None]
    grad_sum = lax.psum(grad_partial[0], "dp").astype(jnp.float32)
    return (mixed, grad_sum)


def solution(mesh):
    placed = (
        P("dp", "mp", None),
        P(),
        P(),
        P(None, None, "mp"),
        P("mp", None),
        P("dp", "mp", None),
    )
    return jax.shard_map(
        functools.partial(body, mesh.shape["mp"]),
        mesh=mesh,
        in_specs=placed,
        out_specs=(P("dp", "mp", None), P("mp", None)),
        check_vma=False,
    )
```
